256 devices in a mesh: blk: 128 (over z, y_lo, x, core), feat: 2 (over y_hi).
Axes of the slice: x: 4, y: 4 (y_hi: 2, y_lo: 2; y = y_hi * 2 + y_lo), z: 8, core: 2. Of those that a mesh axis runs over, the one named last changes fastest.
Arguments:
- samples: float32 [98304, 2048], P('blk', 'feat'), may hold values from -6 to 6
Outputs:
- band: float32 [5, 98304, 768], P(None, 'blk', 'feat')
The draws below stay inside these ranges and needn't reach their ends.
All inputs are finite; a program needn't handle non-finite values.
Results may differ from the reference program's by a relative error of at most 0.0001.
Values sent between devices are 32-bit elements; how exact they have to be, the bound alone decides.
A program may use at most 128 MiB of HBM per device.

```python
import jax
import jax.numpy as jnp
from jax import lax

F = 2048
S_DEV = 768
HALF = 2
SAMPLES = 98304


def shard_levels(key, extent, pieces, low, top_value):
    gain, own = 1.0, jax.random.fold_in(key, 6)
    for position, blocks in pieces:
        heights = jnp.exp(jax.random.uniform(jax.random.fold_in(own, position), (blocks,), jnp.float32, low / len(pieces), top_value / len(pieces)))
        gain = gain * jnp.repeat(heights, extent[position] // blocks).reshape([-1 if axis == position else 1 for axis in range(len(extent))])
    return gain


def gaussian(key, shape, width, reach, shards=(), kind=jnp.bfloat16):
    factor_of = shard_levels(key, shape, shards, -0.22, 0.18) if shards else 1.0
    values = jax.random.normal(key, shape, jnp.float32) * width * factor_of
    return jnp.minimum(jnp.maximum(values, -reach), reach).astype(kind)


def setup_inputs(seed: int = 0) -> dict:
    streams_of = jax.random.split(jax.random.key(seed), 2)
    samples = gaussian(streams_of[0], (SAMPLES, F), 1.0, 6.0, ((0, 128), (1, 2)), jnp.float32)
    return {"samples": samples}


def reference(samples):
    blocks = samples.reshape(-1, S_DEV, F)
    scale = 1.0 / jnp.sqrt(jnp.float32(F))
    results = []
    for index in range(2 * HALF + 1):
        other = jnp.roll(blocks, -(index - HALF), axis=0)
        prod = jnp.einsum('isf,itf->ist', blocks, other, precision=lax.Precision.HIGHEST, preferred_element_type=jnp.float32)
        results.append((prod * scale).reshape(-1, S_DEV))
    return jnp.stack(results)
```

```python
import functools

import jax
import jax.numpy as jnp
from jax import lax
from jax.experimental import pallas as pl
from jax.experimental.pallas import tpu as pltpu
from jax.sharding import PartitionSpec as P

MESH = pl.DeviceIdType.MESH
LANES = 128
NX = 4
PARTS = 2
LEAD = 2
UP, OWN, DOWN = 0, 2, 4


def kernel(blocks, chunks, half, scale, x_ref, out_ref, buf, other, transit, r_hi, r_lo, g_hi, g_lo, r_buf, r_other, r_transit, s_sem):
    blk, f = lax.axis_index("blk"), lax.axis_index("feat")
    core = lax.rem(blk, 2)
    x = lax.rem(blk // 2, NX)
    lo = lax.rem(blk // (2 * NX), 2)
    first, last = 1 - jnp.minimum(x, 1), x // (NX - 1)
    row, plane = 2 * NX, 4 * NX

    def at(index, feat):
        return (lax.rem(index + blocks, blocks), feat)

    near = at(blk + row - 2 * row * lo, f)
    cross = at(blk + row - 2 * row * lo, 1 - f)
    twin = at(blk + 1 - 2 * core, f)
    up = at(blk + 2 - row * last + plane * last * (1 - lo), f)
    down = at(blk - 2 + row * first - plane * first * lo, f)
    up_source = at(blk - 2 + row * first - plane * first * (1 - lo), f)
    down_source = at(blk + 2 - row * last + plane * last * lo, f)
    twin_slot = 3 - 2 * core
    extra_slot = 1 + 2 * core
    passed_slot = 4 - 4 * core
    kept_slot = 4 * core
    part = half // PARTS

    def load(k):
        columns = pl.ds(k * LANES, LANES)
        mine = pl.ds(pl.multiple_of(f * half, half), half)
        rest = pl.ds(pl.multiple_of((1 - f) * half, half), half)
        return (
            pltpu.make_async_copy(x_ref.at[mine, columns], buf.at[OWN, 0, k], r_buf.at[OWN, 0, k, 0]),
            pltpu.make_async_copy(x_ref.at[rest, columns], other.at[0, k], r_other.at[0, k, 0]),
        )

    def send(flow, source, target, arrived, device):
        pltpu.make_async_remote_copy(
            src_ref=source,
            dst_ref=target,
            send_sem=s_sem.at[flow],
            recv_sem=arrived,
            device_id=device,
            device_id_type=MESH,
        ).start()

    def landed(target, arrived):
        pltpu.make_async_remote_copy(
            src_ref=target,
            dst_ref=target,
            send_sem=s_sem.at[0],
            recv_sem=arrived,
            device_id=twin,
            device_id_type=MESH,
        ).wait_recv()

    def rows(r):
        return pl.ds(r * part, part)

    def to_near(source, side, k, r):
        if side == 0:
            send(0, source, transit.at[0, k, rows(r)], r_transit.at[0, k, r], near)
        else:
            send(0, source, buf.at[OWN, 1, k, rows(r)], r_buf.at[OWN, 1, k, r], near)

    def to_cross(source, side, k, r):
        if side == 0:
            send(1, source, transit.at[1, k, rows(r)], r_transit.at[1, k, r], cross)
        else:
            send(1, source, other.at[1, k, rows(r)], r_other.at[1, k, r], cross)

    def to_up(source, side, k, r):
        send(2, source, buf.at[UP, side, k, rows(r)], r_buf.at[UP, side, k, r], up)

    def to_down(source, side, k, r):
        send(3, source, buf.at[DOWN, side, k, rows(r)], r_buf.at[DOWN, side, k, r], down)

    def to_twin(source, side, k, r):
        slot = extra_slot
        send(4, source, buf.at[slot, side, k, rows(r)], r_buf.at[slot, side, k, r], twin)

    def pass_on(side, k, r):
        slot = twin_slot
        source = buf.at[passed_slot, side, k, rows(r)]
        send(5, source, buf.at[slot, side, k, rows(r)], r_buf.at[slot, side, k, r], twin)

    def send_rows(side, k, r):
        source = buf.at[OWN, side, k, rows(r)]

        @pl.when(x < NX - 1)
        def _():
            to_up(source, side, k, r)

        @pl.when(x > 0)
        def _():
            to_down(source, side, k, r)

        to_twin(source, side, k, r)

    def wrap_rows(side, k, r):
        source = transit.at[side, k, rows(r)]

        @pl.when(x == NX - 1)
        def _():
            to_up(source, side, k, r)

        @pl.when(x == 0)
        def _():
            to_down(source, side, k, r)

    def send_own(k):
        for copy in load(k):
            copy.wait()
        for r in range(PARTS):
            to_near(buf.at[OWN, 0, k, rows(r)], 0, k, r)
            to_cross(other.at[0, k, rows(r)], 0, k, r)
            send_rows(0, k, r)

    def load_all(k, carry):
        for copy in load(k):
            copy.start()
        return carry

    lax.fori_loop(0, chunks, load_all, 0)

    barrier = pltpu.get_barrier_semaphore()
    for device in (near, cross, twin, up_source, down_source):
        pl.semaphore_signal(barrier, inc=1, device_id=device, device_id_type=MESH)
    pl.semaphore_wait(barrier, 5)

    for k in range(LEAD):
        send_own(k)

    def clear(b, carry):
        out_ref[b] = jnp.zeros(out_ref.shape[1:], jnp.float32)
        return carry

    lax.fori_loop(0, 5, clear, 0)

    def split(value):
        hi = value.astype(jnp.bfloat16)
        return hi, (value - hi.astype(jnp.float32)).astype(jnp.bfloat16)

    def dot(left, right):
        return lax.dot_general(left, right, (((1,), (1,)), ((), ())), preferred_element_type=jnp.float32)

    def multiply(k):
        for side in range(2):
            columns = pl.ds(side * LANES, LANES)
            g_hi[:, columns], g_lo[:, columns] = split(other[side, k])

        def split_slot(b, carry):
            for side in range(2):
                columns = pl.ds(side * LANES, LANES)
                r_hi[b, :, columns], r_lo[b, :, columns] = split(buf[b, side, k])
            return carry

        lax.fori_loop(0, 5, split_slot, 0)

        def block(b, carry):
            mine = pl.ds(pl.multiple_of(f * half, half), half)
            rest = pl.ds(pl.multiple_of((1 - f) * half, half), half)
            right_hi, right_lo = r_hi[b], r_lo[b]
            for where, left_hi, left_lo in ((mine, r_hi[OWN], r_lo[OWN]), (rest, g_hi[...], g_lo[...])):
                total = dot(left_hi, right_hi) + dot(left_hi, right_lo) + dot(left_lo, right_hi)
                out_ref[b, where] += total * scale
            return carry

        lax.fori_loop(0, 5, block, 0)

    def step(t, carry):
        @pl.when(t < chunks)
        def _():
            for r in range(PARTS):
                landed(transit.at[1, t, rows(r)], r_transit.at[1, t, r])
                to_near(transit.at[1, t, rows(r)], 1, t, r)
                landed(transit.at[0, t, rows(r)], r_transit.at[0, t, r])
                to_cross(transit.at[0, t, rows(r)], 1, t, r)
                wrap_rows(0, t, r)
                wrap_rows(1, t, r)

        @pl.when(jnp.logical_and(t >= 1, t <= chunks))
        def _():
            for r in range(PARTS):
                landed(buf.at[OWN, 1, t - 1, rows(r)], r_buf.at[OWN, 1, t - 1, r])
                send_rows(1, t - 1, r)

        @pl.when(t + LEAD < chunks)
        def _():
            send_own(t + LEAD)

        @pl.when(jnp.logical_and(t >= 2, t <= chunks + 1))
        def _():
            for r in range(PARTS):
                for side in range(2):
                    landed(buf.at[passed_slot, side, t - 2, rows(r)], r_buf.at[passed_slot, side, t - 2, r])
                    pass_on(side, t - 2, r)

        @pl.when(t >= 3)
        def _():
            k = t - 3
            for r in range(PARTS):
                landed(other.at[1, k, rows(r)], r_other.at[1, k, r])
                for side in range(2):
                    for slot in (kept_slot, twin_slot, extra_slot):
                        landed(buf.at[slot, side, k, rows(r)], r_buf.at[slot, side, k, r])
            multiply(k)

        return carry

    lax.fori_loop(0, chunks + 3, step, 0)

    for flow in range(6):
        pltpu.make_async_remote_copy(
            src_ref=transit,
            dst_ref=transit,
            send_sem=s_sem.at[flow],
            recv_sem=r_transit.at[0, 0, 0],
            device_id=twin,
            device_id_type=MESH,
        ).wait_send()


def local(samples):
    count, width = samples.shape
    feats = lax.axis_size("feat")
    half, chunks = count // feats, width // LANES
    scale = float(1.0 / (width * feats) ** 0.5)
    block = (half, LANES)
    return pl.pallas_call(
        functools.partial(kernel, lax.axis_size("blk"), chunks, half, scale),
        out_shape=jax.ShapeDtypeStruct((5, count, half), jnp.float32),
        in_specs=[pl.BlockSpec(memory_space=pltpu.HBM)],
        out_specs=pl.BlockSpec(memory_space=pltpu.VMEM),
        scratch_shapes=[
            pltpu.VMEM((5, 2, chunks, *block), jnp.float32),
            pltpu.VMEM((2, chunks, *block), jnp.float32),
            pltpu.VMEM((2, chunks, *block), jnp.float32),
            pltpu.VMEM((5, half, 2 * LANES), jnp.bfloat16),
            pltpu.VMEM((5, half, 2 * LANES), jnp.bfloat16),
            pltpu.VMEM((half, 2 * LANES), jnp.bfloat16),
            pltpu.VMEM((half, 2 * LANES), jnp.bfloat16),
            pltpu.SemaphoreType.DMA((5, 2, chunks, PARTS)),
            pltpu.SemaphoreType.DMA((2, chunks, PARTS)),
            pltpu.SemaphoreType.DMA((2, chunks, PARTS)),
            pltpu.SemaphoreType.DMA((6,)),
        ],
        compiler_params=pltpu.CompilerParams(collective_id=0, has_side_effects=True, vmem_limit_bytes=63 * 1024 * 1024),
        name="banded_gram",
    )(samples)


def solution(mesh):
    in_specs = (P("blk", "feat"),)
    out_specs = P(None, "blk", "feat")
    return jax.shard_map(local, mesh=mesh, in_specs=in_specs, out_specs=out_specs, check_vma=False)
```

```python
import functools

import jax
import jax.numpy as jnp
from jax import lax
from jax.experimental import pallas as pl
from jax.experimental.pallas import tpu as pltpu
from jax.sharding import PartitionSpec as P

MESH = pl.DeviceIdType.MESH
LANES = 128
NX = 4
PARTS = 2
TILE = 256
ORDER = ("relay", "relay_back", "given", "pass_on", "own_near", "own_cross", "own_rows", "consume")
LATER = dict(own_near=1, own_cross=0, own_rows=1, relay=3, relay_back=4, given=6, pass_on=8, consume=9)
UP, OWN, DOWN = 0, 2, 4


def split(value):
    hi = value.astype(jnp.bfloat16)
    return hi, (value - hi.astype(jnp.float32)).astype(jnp.bfloat16)


def dot(left, right):
    return lax.dot_general(left, right, (((1,), (1,)), ((), ())), preferred_element_type=jnp.float32)


def product(l_hi, l_lo, r_hi, r_lo, where):
    right_hi, right_lo = r_hi[where], r_lo[where]
    return dot(l_hi[...], right_hi) + dot(l_lo[...], right_hi) + dot(l_hi[...], right_lo)


def tiles(width):
    return [pl.ds(start, min(TILE, width - start)) for start in range(0, width, TILE)]


def kernel(blocks, chunks, half, scale, x_ref, acc, r_hi, r_lo, l_hi, l_lo, buf, other, transit, r_buf, r_other, r_transit, s_sem):
    blk, f = lax.axis_index("blk"), lax.axis_index("feat")
    core = lax.rem(blk, 2)
    x = lax.rem(blk // 2, NX)
    lo = lax.rem(blk // (2 * NX), 2)
    first, last = 1 - jnp.minimum(x, 1), x // (NX - 1)
    row, plane = 2 * NX, 4 * NX

    def at(index, feat):
        return (lax.rem(index + blocks, blocks), feat)

    near = at(blk + row - 2 * row * lo, f)
    cross = at(blk + row - 2 * row * lo, 1 - f)
    twin = at(blk + 1 - 2 * core, f)
    up = at(blk + 2 - row * last + plane * last * (1 - lo), f)
    down = at(blk - 2 + row * first - plane * first * lo, f)
    up_source = at(blk - 2 + row * first - plane * first * (1 - lo), f)
    down_source = at(blk + 2 - row * last + plane * last * lo, f)
    twin_slot = 3 - 2 * core
    extra_slot = 1 + 2 * core
    passed_slot = 4 - 4 * core
    kept_slot = 4 * core
    part = half // PARTS

    def rows(r):
        return pl.ds(pl.multiple_of(r * part, part), part)

    def load_mine(k, r):
        source = x_ref.at[pl.ds(pl.multiple_of(f * half + r * part, part), part), pl.ds(pl.multiple_of(k * LANES, LANES), LANES)]
        return pltpu.make_async_copy(source, buf.at[OWN, 0, k, rows(r)], r_buf.at[OWN, 0, k, r])

    def load_rest(k, r):
        source = x_ref.at[pl.ds(pl.multiple_of((1 - f) * half + r * part, part), part), pl.ds(pl.multiple_of(k * LANES, LANES), LANES)]
        return pltpu.make_async_copy(source, other.at[0, k, rows(r)], r_other.at[0, k, r])

    def send(flow, source, target, arrived, device):
        pltpu.make_async_remote_copy(
            src_ref=source,
            dst_ref=target,
            send_sem=s_sem.at[flow],
            recv_sem=arrived,
            device_id=device,
            device_id_type=MESH,
        ).start()

    def landed(target, arrived):
        pltpu.make_async_remote_copy(
            src_ref=target,
            dst_ref=target,
            send_sem=s_sem.at[0],
            recv_sem=arrived,
            device_id=twin,
            device_id_type=MESH,
        ).wait_recv()

    def to_near(source, side, k, r):
        if side == 0:
            send(0, source, transit.at[0, k, rows(r)], r_transit.at[0, k, r], near)
        else:
            send(0, source, buf.at[OWN, 1, k, rows(r)], r_buf.at[OWN, 1, k, r], near)

    def to_cross(source, side, k, r):
        if side == 0:
            send(1, source, transit.at[1, k, rows(r)], r_transit.at[1, k, r], cross)
        else:
            send(1, source, other.at[1, k, rows(r)], r_other.at[1, k, r], cross)

    def to_up(source, side, k, r):
        send(2, source, buf.at[UP, side, k, rows(r)], r_buf.at[UP, side, k, r], up)

    def to_down(source, side, k, r):
        send(3, source, buf.at[DOWN, side, k, rows(r)], r_buf.at[DOWN, side, k, r], down)

    def to_twin(source, side, k, r):
        slot = extra_slot
        send(4, source, buf.at[slot, side, k, rows(r)], r_buf.at[slot, side, k, r], twin)

    def pass_on(side, k, r):
        slot = twin_slot
        source = buf.at[passed_slot, side, k, rows(r)]
        send(5, source, buf.at[slot, side, k, rows(r)], r_buf.at[slot, side, k, r], twin)

    def send_rows(side, k, r):
        source = buf.at[OWN, side, k, rows(r)]

        @pl.when(x < NX - 1)
        def _():
            to_up(source, side, k, r)

        @pl.when(x > 0)
        def _():
            to_down(source, side, k, r)

        to_twin(source, side, k, r)

    def wrap_rows(side, k, r):
        source = transit.at[side, k, rows(r)]

        @pl.when(x == NX - 1)
        def _():
            to_up(source, side, k, r)

        @pl.when(x == 0)
        def _():
            to_down(source, side, k, r)

    def load_all(q, carry):
        k, r = q // PARTS, lax.rem(q, PARTS)
        load_mine(k, r).start()
        load_rest(k, r).start()
        return carry

    lax.fori_loop(0, chunks * PARTS, load_all, 0)

    barrier = pltpu.get_barrier_semaphore()
    for device in (near, cross, twin, up_source, down_source):
        pl.semaphore_signal(barrier, inc=1, device_id=device, device_id_type=MESH)
    pl.semaphore_wait(barrier, 5)

    acc[...] = jnp.zeros_like(acc)

    def turn(name):
        return LATER[name], ORDER.index(name)

    mine_first = "own_near" if turn("own_near") < turn("own_rows") else "own_rows"

    def own_near(k, r):
        if mine_first == "own_near":
            load_mine(k, r).wait()
        to_near(buf.at[OWN, 0, k, rows(r)], 0, k, r)

    def own_rows(k, r):
        if mine_first == "own_rows":
            load_mine(k, r).wait()
        send_rows(0, k, r)

    def own_cross(k, r):
        load_rest(k, r).wait()
        to_cross(other.at[0, k, rows(r)], 0, k, r)

    def relay(k, r):
        landed(transit.at[1, k, rows(r)], r_transit.at[1, k, r])
        to_near(transit.at[1, k, rows(r)], 1, k, r)
        wrap_rows(1, k, r)

    def relay_back(k, r):
        landed(transit.at[0, k, rows(r)], r_transit.at[0, k, r])
        to_cross(transit.at[0, k, rows(r)], 1, k, r)
        wrap_rows(0, k, r)

    def given(k, r):
        landed(buf.at[OWN, 1, k, rows(r)], r_buf.at[OWN, 1, k, r])
        send_rows(1, k, r)

    def pass_on_both(k, r):
        for side in range(2):
            landed(buf.at[passed_slot, side, k, rows(r)], r_buf.at[passed_slot, side, k, r])
            pass_on(side, k, r)

    def split_chunk(k):
        mine = pl.ds(pl.multiple_of(f * half, half), half)
        rest = pl.ds(pl.multiple_of((1 - f) * half, half), half)
        for side in range(2):
            columns = pl.ds(side * LANES, LANES)
            l_hi[mine, columns], l_lo[mine, columns] = split(buf[OWN, side, k])
            l_hi[rest, columns], l_lo[rest, columns] = split(other[side, k])

        def split_slot(b, carry):
            where = pl.ds(pl.multiple_of(b * half, half), half)
            for side in range(2):
                columns = pl.ds(side * LANES, LANES)
                r_hi[where, columns], r_lo[where, columns] = split(buf[b, side, k])
            return carry

        lax.fori_loop(0, 5, split_slot, 0)

    every = tiles(acc.shape[1])
    share = -(-len(every) // PARTS)

    def consume(k, r):
        landed(other.at[1, k, rows(r)], r_other.at[1, k, r])
        for side in range(2):
            for slot in (kept_slot, twin_slot, extra_slot):
                landed(buf.at[slot, side, k, rows(r)], r_buf.at[slot, side, k, r])

        @pl.when(r == PARTS - 1)
        def _():
            split_chunk(k)

        for turn_ in range(PARTS):
            ready = jnp.logical_and(r == PARTS - 1, k < chunks - 1) if turn_ == 0 else jnp.logical_and(r == turn_ - 1, k > 0)

            @pl.when(ready)
            def _(turn_=turn_):
                for where in every[turn_ * share : (turn_ + 1) * share]:
                    acc[:, where] += product(l_hi, l_lo, r_hi, r_lo, where) * scale

    actions = dict(
        own_near=own_near,
        own_rows=own_rows,
        own_cross=own_cross,
        relay=relay,
        relay_back=relay_back,
        given=given,
        pass_on=pass_on_both,
        consume=consume,
    )
    count = chunks * PARTS

    def step(t, carry):
        for name in ORDER:
            q = t - LATER[name]

            @pl.when(jnp.logical_and(q >= 0, q < count))
            def _(name=name, q=q):
                actions[name](q // PARTS, lax.rem(q, PARTS))

        return carry

    lax.fori_loop(0, count + max(LATER.values()), step, 0)

    for flow in range(6):
        pltpu.make_async_remote_copy(
            src_ref=transit,
            dst_ref=transit,
            send_sem=s_sem.at[flow],
            recv_sem=r_transit.at[0, 0, 0],
            device_id=twin,
            device_id_type=MESH,
        ).wait_send()


def finish(half, scale, acc, r_hi, r_lo, l_hi, l_lo, out_ref, total, sem):
    copies = [pltpu.make_async_copy(total.at[:, pl.ds(b * half, half)], out_ref.at[b], sem.at[b]) for b in range(5)]
    started = 0
    for where in tiles(acc.shape[1]):
        total[:, where] = acc[:, where] + product(l_hi, l_lo, r_hi, r_lo, where) * scale
        while (started + 1) * half <= where.start + where.size:
            copies[started].start()
            started += 1
    for copy in copies:
        copy.wait()


def local(samples):
    count, width = samples.shape
    feats = lax.axis_size("feat")
    half, chunks = count // feats, width // LANES
    scale = float(1.0 / (width * feats) ** 0.5)
    block = (half, LANES)
    parts = pl.pallas_call(
        functools.partial(kernel, lax.axis_size("blk"), chunks, half, scale),
        out_shape=[
            pltpu.VMEM((count, 5 * half), jnp.float32),
            pltpu.VMEM((5 * half, 2 * LANES), jnp.bfloat16),
            pltpu.VMEM((5 * half, 2 * LANES), jnp.bfloat16),
            pltpu.VMEM((count, 2 * LANES), jnp.bfloat16),
            pltpu.VMEM((count, 2 * LANES), jnp.bfloat16),
        ],
        in_specs=[pl.BlockSpec(memory_space=pltpu.HBM)],
        out_specs=[pl.BlockSpec(memory_space=pltpu.VMEM)] * 5,
        scratch_shapes=[
            pltpu.VMEM((5, 2, chunks, *block), jnp.float32),
            pltpu.VMEM((2, chunks, *block), jnp.float32),
            pltpu.VMEM((2, chunks, *block), jnp.float32),
            pltpu.SemaphoreType.DMA((5, 2, chunks, PARTS)),
            pltpu.SemaphoreType.DMA((2, chunks, PARTS)),
            pltpu.SemaphoreType.DMA((2, chunks, PARTS)),
            pltpu.SemaphoreType.DMA((6,)),
        ],
        compiler_params=pltpu.CompilerParams(collective_id=0, has_side_effects=True, vmem_limit_bytes=54 * 1024 * 1024),
        name="banded_gram",
    )(samples)
    return pl.pallas_call(
        functools.partial(finish, half, scale),
        out_shape=jax.ShapeDtypeStruct((5, count, half), jnp.float32),
        in_specs=[pl.BlockSpec(memory_space=pltpu.VMEM)] * 5,
        out_specs=pl.BlockSpec(memory_space=pltpu.HBM),
        scratch_shapes=[pltpu.VMEM((count, 5 * half), jnp.float32), pltpu.SemaphoreType.DMA((5,))],
        compiler_params=pltpu.CompilerParams(vmem_limit_bytes=16 * 1024 * 1024),
        name="finish",
    )(*parts)


def solution(mesh):
    in_specs = (P("blk", "feat"),)
    out_specs = P(None, "blk", "feat")
    return jax.shard_map(local, mesh=mesh, in_specs=in_specs, out_specs=out_specs, check_vma=False)
```

```python
import functools

import jax
import jax.numpy as jnp
from jax import lax
from jax.experimental import pallas as pl
from jax.experimental.pallas import tpu as pltpu
from jax.sharding import PartitionSpec as P

MESH = pl.DeviceIdType.MESH
LANES = 128
NX = 4
PARTS = 2
TILE = 256
ORDER = ("relay", "relay_back", "wrap_late", "given", "pass_on", "clear", "own_near", "own_cross", "own_rows", "consume")
LATER = dict(clear=4, wrap_late=6, own_near=1, own_cross=0, own_rows=1, relay=3, relay_back=4, given=6, pass_on=8, consume=9)
UP, OWN, DOWN = 0, 2, 4


def split(value):
    hi = value.astype(jnp.bfloat16)
    return hi, (value - hi.astype(jnp.float32)).astype(jnp.bfloat16)


def dot(left, right):
    return lax.dot_general(left, right, (((1,), (1,)), ((), ())), preferred_element_type=jnp.float32)


def product(l_hi, l_lo, r_hi, r_lo, where):
    right_hi, right_lo = r_hi[where], r_lo[where]
    return dot(l_hi[...], right_hi) + dot(l_lo[...], right_hi) + dot(l_hi[...], right_lo)


def tiles(width):
    return [pl.ds(start, min(TILE, width - start)) for start in range(0, width, TILE)]


def early_tiles(width, half):
    clear = lambda where, b: where.start + where.size <= b * half or where.start >= (b + 1) * half
    return [where for where in tiles(width) if clear(where, 1) and clear(where, 3)]


def kernel(blocks, chunks, half, scale, x_ref, acc, r_hi, r_lo, l_hi, l_lo, buf, other, transit, r_buf, r_other, r_transit, s_sem, ready):
    blk, f = lax.axis_index("blk"), lax.axis_index("feat")
    core = lax.rem(blk, 2)
    x = lax.rem(blk // 2, NX)
    lo = lax.rem(blk // (2 * NX), 2)
    first, last = 1 - jnp.minimum(x, 1), x // (NX - 1)
    row, plane = 2 * NX, 4 * NX
    crosses, crossed = first * lo, last * lo
    late = crosses * (1 - jnp.minimum(blk // plane, 1))

    def at(index, feat):
        return (lax.rem(index + blocks, blocks), feat)

    near = at(blk + row - 2 * row * lo, f)
    cross = at(blk + row - 2 * row * lo, 1 - f)
    twin = at(blk + 1 - 2 * core, f)
    up = at(blk + 2 - row * last + plane * last * (1 - lo), f)
    down = at(blk - 2 + row * first - plane * first * lo, f)
    up_source = at(blk - 2 + row * first - plane * first * (1 - lo), f)
    down_source = at(blk + 2 - row * last + plane * last * lo, f)
    twin_slot = 3 - 2 * core
    extra_slot = 1 + 2 * core
    passed_slot = 4 - 4 * core
    kept_slot = 4 * core
    part = half // PARTS

    def rows(r):
        return pl.ds(pl.multiple_of(r * part, part), part)

    def load_mine(k, r):
        source = x_ref.at[pl.ds(pl.multiple_of(f * half + r * part, part), part), pl.ds(pl.multiple_of(k * LANES, LANES), LANES)]
        return pltpu.make_async_copy(source, buf.at[OWN, 0, k, rows(r)], r_buf.at[OWN, 0, k, r])

    def load_rest(k, r):
        source = x_ref.at[pl.ds(pl.multiple_of((1 - f) * half + r * part, part), part), pl.ds(pl.multiple_of(k * LANES, LANES), LANES)]
        return pltpu.make_async_copy(source, other.at[0, k, rows(r)], r_other.at[0, k, r])

    def send(flow, source, target, arrived, device):
        pltpu.make_async_remote_copy(
            src_ref=source,
            dst_ref=target,
            send_sem=s_sem.at[flow],
            recv_sem=arrived,
            device_id=device,
            device_id_type=MESH,
        ).start()

    def landed(target, arrived):
        pltpu.make_async_remote_copy(
            src_ref=target,
            dst_ref=target,
            send_sem=s_sem.at[0],
            recv_sem=arrived,
            device_id=twin,
            device_id_type=MESH,
        ).wait_recv()

    def to_near(source, side, k, r):
        if side == 0:
            send(0, source, transit.at[0, k, rows(r)], r_transit.at[0, k, r], near)
        else:
            send(0, source, buf.at[OWN, 1, k, rows(r)], r_buf.at[OWN, 1, k, r], near)

    def to_cross(source, side, k, r):
        if side == 0:
            send(1, source, transit.at[1, k, rows(r)], r_transit.at[1, k, r], cross)
        else:
            send(1, source, other.at[1, k, rows(r)], r_other.at[1, k, r], cross)

    def to_up(source, side, k, r):
        send(2, source, buf.at[UP, side, k, rows(r)], r_buf.at[UP, side, k, r], up)

    def to_down(source, side, k, r):
        send(3, source, buf.at[DOWN, side, k, rows(r)], r_buf.at[DOWN, side, k, r], down)

    def to_twin(source, side, k, r):
        slot = extra_slot
        send(4, source, buf.at[slot, side, k, rows(r)], r_buf.at[slot, side, k, r], twin)

    def pass_on(side, k, r):
        slot = twin_slot
        source = buf.at[passed_slot, side, k, rows(r)]
        send(5, source, buf.at[slot, side, k, rows(r)], r_buf.at[slot, side, k, r], twin)

    def send_rows(side, k, r):
        source = buf.at[OWN, side, k, rows(r)]

        @pl.when(x < NX - 1)
        def _():
            to_up(source, side, k, r)

        @pl.when(x > 0)
        def _():
            to_down(source, side, k, r)

        to_twin(source, side, k, r)

    def wrap_down(side, k, r):
        to_down(transit.at[side, k, rows(r)], side, k, r)

    def wait_ready(k, r, when):
        @pl.when(jnp.logical_and(when, k * PARTS + r == 0))
        def _():
            pl.semaphore_wait(ready, 1)

    def wrap_rows(side, k, r):
        @pl.when(x == NX - 1)
        def _():
            to_up(transit.at[side, k, rows(r)], side, k, r)

        @pl.when(jnp.logical_and(x == 0, late == 0))
        def _():
            wrap_down(side, k, r)

    def wrap_late(k, r):
        wait_ready(k, r, late == 1)

        @pl.when(late == 1)
        def _():
            for side in range(2):
                wrap_down(side, k, r)

    def load_all(q, carry):
        k, r = q // PARTS, lax.rem(q, PARTS)
        load_mine(k, r).start()
        load_rest(k, r).start()
        return carry

    lax.fori_loop(0, chunks * PARTS, load_all, 0)

    barrier = pltpu.get_barrier_semaphore()
    def greet(device):
        pl.semaphore_signal(barrier, inc=1, device_id=device, device_id_type=MESH)

    for device in (near, cross, twin, up_source):
        greet(device)

    @pl.when(crossed == 0)
    def _():
        greet(down_source)

    @pl.when(crosses == 1)
    def _():
        greet(down)

    pl.semaphore_wait(barrier, 5 - crosses + crossed)

    @pl.when(crossed == 1)
    def _():
        pl.semaphore_signal(ready, inc=1, device_id=down_source, device_id_type=MESH)

    def turn(name):
        return LATER[name], ORDER.index(name)

    wrap_first = "relay" if turn("relay") < turn("relay_back") else "relay_back"
    in_time = jnp.logical_and(crosses == 1, late == 0)
    mine_first = "own_near" if turn("own_near") < turn("own_rows") else "own_rows"

    def clear(k, r):
        @pl.when(k * PARTS + r == 0)
        def _():
            acc[...] = jnp.zeros_like(acc)

    def own_near(k, r):
        if mine_first == "own_near":
            load_mine(k, r).wait()
        to_near(buf.at[OWN, 0, k, rows(r)], 0, k, r)

    def own_rows(k, r):
        if mine_first == "own_rows":
            load_mine(k, r).wait()
        send_rows(0, k, r)

    def own_cross(k, r):
        load_rest(k, r).wait()
        to_cross(other.at[0, k, rows(r)], 0, k, r)

    def relay(k, r):
        landed(transit.at[1, k, rows(r)], r_transit.at[1, k, r])
        to_near(transit.at[1, k, rows(r)], 1, k, r)
        if wrap_first == "relay":
            wait_ready(k, r, in_time)
        wrap_rows(1, k, r)

    def relay_back(k, r):
        landed(transit.at[0, k, rows(r)], r_transit.at[0, k, r])
        to_cross(transit.at[0, k, rows(r)], 1, k, r)
        if wrap_first == "relay_back":
            wait_ready(k, r, in_time)
        wrap_rows(0, k, r)

    def given(k, r):
        landed(buf.at[OWN, 1, k, rows(r)], r_buf.at[OWN, 1, k, r])
        send_rows(1, k, r)

    def pass_on_both(k, r):
        for side in range(2):
            landed(buf.at[passed_slot, side, k, rows(r)], r_buf.at[passed_slot, side, k, r])
            pass_on(side, k, r)

    def split_left(k):
        mine = pl.ds(pl.multiple_of(f * half, half), half)
        rest = pl.ds(pl.multiple_of((1 - f) * half, half), half)
        for side in range(2):
            columns = pl.ds(side * LANES, LANES)
            l_hi[mine, columns], l_lo[mine, columns] = split(buf[OWN, side, k])
            l_hi[rest, columns], l_lo[rest, columns] = split(other[side, k])

    def split_slot(b, k):
        where = pl.ds(pl.multiple_of(b * half, half), half)
        for side in range(2):
            columns = pl.ds(side * LANES, LANES)
            r_hi[where, columns], r_lo[where, columns] = split(buf[b, side, k])

    def split_slots(k):
        def one(b, carry):
            @pl.when(b != extra_slot)
            def _():
                split_slot(b, k)

            return carry

        lax.fori_loop(0, 5, one, 0)

    every = tiles(acc.shape[1])
    share = -(-len(every) // PARTS)
    early = early_tiles(acc.shape[1], half)

    def add(wheres):
        for where in wheres:
            acc[:, where] += product(l_hi, l_lo, r_hi, r_lo, where) * scale

    def consume(k, r):
        complete = r == PARTS - 1
        landed(other.at[1, k, rows(r)], r_other.at[1, k, r])
        for side in range(2):
            for slot in (kept_slot, twin_slot):
                landed(buf.at[slot, side, k, rows(r)], r_buf.at[slot, side, k, r])

        @pl.when(complete)
        def _():
            split_left(k)
            split_slots(k)

        @pl.when(jnp.logical_and(complete, k == chunks - 1))
        def _():
            add(early)

        for side in range(2):
            landed(buf.at[extra_slot, side, k, rows(r)], r_buf.at[extra_slot, side, k, r])

        @pl.when(complete)
        def _():
            split_slot(extra_slot, k)

        for turn_ in range(PARTS):
            ready_ = jnp.logical_and(complete, k < chunks - 1) if turn_ == 0 else jnp.logical_and(r == turn_ - 1, k > 0)

            @pl.when(ready_)
            def _(turn_=turn_):
                add(every[turn_ * share : (turn_ + 1) * share])

    actions = dict(
        own_near=own_near,
        own_rows=own_rows,
        own_cross=own_cross,
        relay=relay,
        relay_back=relay_back,
        wrap_late=wrap_late,
        given=given,
        pass_on=pass_on_both,
        consume=consume,
        clear=clear,
    )
    count = chunks * PARTS

    def step(t, carry):
        for name in ORDER:
            q = t - LATER[name]

            @pl.when(jnp.logical_and(q >= 0, q < count))
            def _(name=name, q=q):
                actions[name](q // PARTS, lax.rem(q, PARTS))

        return carry

    lax.fori_loop(0, count + max(LATER.values()), step, 0)

    for flow in range(6):
        pltpu.make_async_remote_copy(
            src_ref=transit,
            dst_ref=transit,
            send_sem=s_sem.at[flow],
            recv_sem=r_transit.at[0, 0, 0],
            device_id=twin,
            device_id_type=MESH,
        ).wait_send()


def finish(half, scale, acc, r_hi, r_lo, l_hi, l_lo, out_ref, total, sem):
    every = tiles(acc.shape[1])
    early = early_tiles(acc.shape[1], half)
    copies = []

    def write(source, where):
        for b in range(5):
            start, stop = max(where.start, b * half), min(where.start + where.size, (b + 1) * half)
            if start < stop:
                target = out_ref.at[b, :, pl.ds(start - b * half, stop - start)]
                copies.append(pltpu.make_async_copy(source.at[:, pl.ds(start, stop - start)], target, sem.at[len(copies)]))
                copies[-1].start()

    for where in every:
        if where in early:
            write(acc, where)
    for where in every:
        if where not in early:
            total[:, where] = acc[:, where] + product(l_hi, l_lo, r_hi, r_lo, where) * scale
            write(total, where)
    for copy in copies:
        copy.wait()


def local(samples):
    count, width = samples.shape
    feats = lax.axis_size("feat")
    half, chunks = count // feats, width // LANES
    scale = float(1.0 / (width * feats) ** 0.5)
    block = (half, LANES)
    parts = pl.pallas_call(
        functools.partial(kernel, lax.axis_size("blk"), chunks, half, scale),
        out_shape=[
            pltpu.VMEM((count, 5 * half), jnp.float32),
            pltpu.VMEM((5 * half, 2 * LANES), jnp.bfloat16),
            pltpu.VMEM((5 * half, 2 * LANES), jnp.bfloat16),
            pltpu.VMEM((count, 2 * LANES), jnp.bfloat16),
            pltpu.VMEM((count, 2 * LANES), jnp.bfloat16),
        ],
        in_specs=[pl.BlockSpec(memory_space=pltpu.HBM)],
        out_specs=[pl.BlockSpec(memory_space=pltpu.VMEM)] * 5,
        scratch_shapes=[
            pltpu.VMEM((5, 2, chunks, *block), jnp.float32),
            pltpu.VMEM((2, chunks, *block), jnp.float32),
            pltpu.VMEM((2, chunks, *block), jnp.float32),
            pltpu.SemaphoreType.DMA((5, 2, chunks, PARTS)),
            pltpu.SemaphoreType.DMA((2, chunks, PARTS)),
            pltpu.SemaphoreType.DMA((2, chunks, PARTS)),
            pltpu.SemaphoreType.DMA((6,)),
            pltpu.SemaphoreType.REGULAR,
        ],
        compiler_params=pltpu.CompilerParams(collective_id=0, has_side_effects=True, vmem_limit_bytes=54 * 1024 * 1024),
        name="banded_gram",
    )(samples)
    return pl.pallas_call(
        functools.partial(finish, half, scale),
        out_shape=jax.ShapeDtypeStruct((5, count, half), jnp.float32),
        in_specs=[pl.BlockSpec(memory_space=pltpu.VMEM)] * 5,
        out_specs=pl.BlockSpec(memory_space=pltpu.HBM),
        scratch_shapes=[pltpu.VMEM((count, 5 * half), jnp.float32), pltpu.SemaphoreType.DMA((16,))],
        compiler_params=pltpu.CompilerParams(vmem_limit_bytes=16 * 1024 * 1024),
        name="finish",
    )(*parts)


def solution(mesh):
    in_specs = (P("blk", "feat"),)
    out_specs = P(None, "blk", "feat")
    return jax.shard_map(local, mesh=mesh, in_specs=in_specs, out_specs=out_specs, check_vma=False)
```

```python
import functools

import jax
import jax.numpy as jnp
from jax import lax
from jax.experimental import pallas as pl
from jax.experimental.pallas import tpu as pltpu
from jax.sharding import PartitionSpec as P

MESH = pl.DeviceIdType.MESH
LANES = 128
NX = 4
PARTS = 2
TILE = 256
ORDER = ("relay", "relay_back", "wrap_late", "given", "pass_on", "clear", "own_near", "own_cross", "own_rows", "consume")
LATER = dict(own_near=1, own_cross=0, own_rows=1, relay=2, relay_back=3, wrap_late=5, given=4, pass_on=6, consume=7, clear=4)
UP, OWN, DOWN = 0, 2, 4


def split(value):
    hi = value.astype(jnp.bfloat16)
    return hi, (value - hi.astype(jnp.float32)).astype(jnp.bfloat16)


def dot(left, right):
    return lax.dot_general(left, right, (((1,), (1,)), ((), ())), preferred_element_type=jnp.float32)


def product(l_hi, l_lo, r_hi, r_lo, where):
    right_hi, right_lo = r_hi[where], r_lo[where]
    return dot(l_hi[...], right_hi) + dot(l_lo[...], right_hi) + dot(l_hi[...], right_lo)


def tiles(width):
    return [pl.ds(start, min(TILE, width - start)) for start in range(0, width, TILE)]


def early_tiles(width, half):
    clear = lambda where, b: where.start + where.size <= b * half or where.start >= (b + 1) * half
    return [where for where in tiles(width) if clear(where, 1) and clear(where, 3)]


def kernel(blocks, chunks, half, scale, x_ref, acc, r_hi, r_lo, l_hi, l_lo, buf, other, transit, r_buf, r_other, r_transit, s_sem, ready):
    blk, f = lax.axis_index("blk"), lax.axis_index("feat")
    core = lax.rem(blk, 2)
    x = lax.rem(blk // 2, NX)
    lo = lax.rem(blk // (2 * NX), 2)
    first, last = 1 - jnp.minimum(x, 1), x // (NX - 1)
    row, plane = 2 * NX, 4 * NX
    crosses, crossed = first * lo, last * lo
    late = crosses * (1 - jnp.minimum(blk // plane, 1))

    def at(index, feat):
        return (lax.rem(index + blocks, blocks), feat)

    near = at(blk + row - 2 * row * lo, f)
    cross = at(blk + row - 2 * row * lo, 1 - f)
    twin = at(blk + 1 - 2 * core, f)
    up = at(blk + 2 - row * last + plane * last * (1 - lo), f)
    down = at(blk - 2 + row * first - plane * first * lo, f)
    up_source = at(blk - 2 + row * first - plane * first * (1 - lo), f)
    down_source = at(blk + 2 - row * last + plane * last * lo, f)
    twin_slot = 3 - 2 * core
    extra_slot = 1 + 2 * core
    passed_slot = 4 - 4 * core
    kept_slot = 4 * core
    part = half // PARTS

    def rows(r):
        return pl.ds(pl.multiple_of(r * part, part), part)

    def load_mine(k, r):
        source = x_ref.at[pl.ds(pl.multiple_of(f * half + r * part, part), part), pl.ds(pl.multiple_of(k * LANES, LANES), LANES)]
        return pltpu.make_async_copy(source, buf.at[OWN, 0, k, rows(r)], r_buf.at[OWN, 0, k, r])

    def load_rest(k, r):
        source = x_ref.at[pl.ds(pl.multiple_of((1 - f) * half + r * part, part), part), pl.ds(pl.multiple_of(k * LANES, LANES), LANES)]
        return pltpu.make_async_copy(source, other.at[0, k, rows(r)], r_other.at[0, k, r])

    def send(flow, source, target, arrived, device):
        pltpu.make_async_remote_copy(
            src_ref=source,
            dst_ref=target,
            send_sem=s_sem.at[flow],
            recv_sem=arrived,
            device_id=device,
            device_id_type=MESH,
        ).start()

    def landed(target, arrived):
        pltpu.make_async_remote_copy(
            src_ref=target,
            dst_ref=target,
            send_sem=s_sem.at[0],
            recv_sem=arrived,
            device_id=twin,
            device_id_type=MESH,
        ).wait_recv()

    def to_near(source, side, k, r):
        if side == 0:
            send(0, source, transit.at[0, k, rows(r)], r_transit.at[0, k, r], near)
        else:
            send(0, source, buf.at[OWN, 1, k, rows(r)], r_buf.at[OWN, 1, k, r], near)

    def to_cross(source, side, k, r):
        if side == 0:
            send(1, source, transit.at[1, k, rows(r)], r_transit.at[1, k, r], cross)
        else:
            send(1, source, other.at[1, k, rows(r)], r_other.at[1, k, r], cross)

    def to_up(source, side, k, r):
        send(2, source, buf.at[UP, side, k, rows(r)], r_buf.at[UP, side, k, r], up)

    def to_down(source, side, k, r):
        send(3, source, buf.at[DOWN, side, k, rows(r)], r_buf.at[DOWN, side, k, r], down)

    def to_twin(source, side, k, r):
        slot = extra_slot
        send(4, source, buf.at[slot, side, k, rows(r)], r_buf.at[slot, side, k, r], twin)

    def pass_on(side, k, r):
        slot = twin_slot
        source = buf.at[passed_slot, side, k, rows(r)]
        send(5, source, buf.at[slot, side, k, rows(r)], r_buf.at[slot, side, k, r], twin)

    def send_rows(side, k, r):
        source = buf.at[OWN, side, k, rows(r)]

        @pl.when(x < NX - 1)
        def _():
            to_up(source, side, k, r)

        @pl.when(x > 0)
        def _():
            to_down(source, side, k, r)

        to_twin(source, side, k, r)

    def wrap_down(side, k, r):
        to_down(transit.at[side, k, rows(r)], side, k, r)

    def wait_ready(k, r, when):
        @pl.when(jnp.logical_and(when, k * PARTS + r == 0))
        def _():
            pl.semaphore_wait(ready, 1)

    def wrap_rows(side, k, r):
        @pl.when(x == NX - 1)
        def _():
            to_up(transit.at[side, k, rows(r)], side, k, r)

        @pl.when(jnp.logical_and(x == 0, late == 0))
        def _():
            wrap_down(side, k, r)

    def wrap_late(k, r):
        wait_ready(k, r, late == 1)

        @pl.when(late == 1)
        def _():
            for side in range(2):
                wrap_down(side, k, r)

    def load_all(q, carry):
        k, r = q // PARTS, lax.rem(q, PARTS)
        load_mine(k, r).start()
        load_rest(k, r).start()
        return carry

    barrier = pltpu.get_barrier_semaphore()
    def greet(device):
        pl.semaphore_signal(barrier, inc=1, device_id=device, device_id_type=MESH)

    for device in (near, cross, twin, up_source):
        greet(device)

    @pl.when(crossed == 0)
    def _():
        greet(down_source)

    @pl.when(crosses == 1)
    def _():
        greet(down)

    lax.fori_loop(0, chunks * PARTS, load_all, 0)

    pl.semaphore_wait(barrier, 5 - crosses + crossed)

    @pl.when(crossed == 1)
    def _():
        pl.semaphore_signal(ready, inc=1, device_id=down_source, device_id_type=MESH)

    def turn(name):
        return LATER[name], ORDER.index(name)

    wrap_first = "relay" if turn("relay") < turn("relay_back") else "relay_back"
    in_time = jnp.logical_and(crosses == 1, late == 0)
    mine_first = "own_near" if turn("own_near") < turn("own_rows") else "own_rows"

    def clear(k, r):
        @pl.when(k * PARTS + r == 0)
        def _():
            acc[...] = jnp.zeros_like(acc)

    def own_near(k, r):
        if mine_first == "own_near":
            load_mine(k, r).wait()
        to_near(buf.at[OWN, 0, k, rows(r)], 0, k, r)

    def own_rows(k, r):
        if mine_first == "own_rows":
            load_mine(k, r).wait()
        send_rows(0, k, r)

    def own_cross(k, r):
        load_rest(k, r).wait()
        to_cross(other.at[0, k, rows(r)], 0, k, r)

    def relay(k, r):
        landed(transit.at[1, k, rows(r)], r_transit.at[1, k, r])
        to_near(transit.at[1, k, rows(r)], 1, k, r)
        if wrap_first == "relay":
            wait_ready(k, r, in_time)
        wrap_rows(1, k, r)

    def relay_back(k, r):
        landed(transit.at[0, k, rows(r)], r_transit.at[0, k, r])
        to_cross(transit.at[0, k, rows(r)], 1, k, r)
        if wrap_first == "relay_back":
            wait_ready(k, r, in_time)
        wrap_rows(0, k, r)

    def given(k, r):
        landed(buf.at[OWN, 1, k, rows(r)], r_buf.at[OWN, 1, k, r])
        send_rows(1, k, r)

    def pass_on_both(k, r):
        for side in range(2):
            landed(buf.at[passed_slot, side, k, rows(r)], r_buf.at[passed_slot, side, k, r])
            pass_on(side, k, r)

    def split_left(k):
        mine = pl.ds(pl.multiple_of(f * half, half), half)
        rest = pl.ds(pl.multiple_of((1 - f) * half, half), half)
        for side in range(2):
            columns = pl.ds(side * LANES, LANES)
            l_hi[mine, columns], l_lo[mine, columns] = split(buf[OWN, side, k])
            l_hi[rest, columns], l_lo[rest, columns] = split(other[side, k])

    def split_slot(b, k):
        where = pl.ds(pl.multiple_of(b * half, half), half)
        for side in range(2):
            columns = pl.ds(side * LANES, LANES)
            r_hi[where, columns], r_lo[where, columns] = split(buf[b, side, k])

    def split_slots(k):
        def one(b, carry):
            @pl.when(b != extra_slot)
            def _():
                split_slot(b, k)

            return carry

        lax.fori_loop(0, 5, one, 0)

    every = tiles(acc.shape[1])
    share = -(-len(every) // PARTS)
    early = early_tiles(acc.shape[1], half)

    def add(wheres):
        for where in wheres:
            acc[:, where] += product(l_hi, l_lo, r_hi, r_lo, where) * scale

    def consume(k, r):
        complete = r == PARTS - 1
        landed(other.at[1, k, rows(r)], r_other.at[1, k, r])
        for side in range(2):
            for slot in (kept_slot, twin_slot):
                landed(buf.at[slot, side, k, rows(r)], r_buf.at[slot, side, k, r])

        @pl.when(complete)
        def _():
            split_left(k)
            split_slots(k)

        @pl.when(jnp.logical_and(complete, k == chunks - 1))
        def _():
            add(early)

        for side in range(2):
            landed(buf.at[extra_slot, side, k, rows(r)], r_buf.at[extra_slot, side, k, r])

        @pl.when(complete)
        def _():
            split_slot(extra_slot, k)

        for turn_ in range(PARTS):
            ready_ = jnp.logical_and(complete, k < chunks - 1) if turn_ == 0 else jnp.logical_and(r == turn_ - 1, k > 0)

            @pl.when(ready_)
            def _(turn_=turn_):
                add(every[turn_ * share : (turn_ + 1) * share])

    actions = dict(
        own_near=own_near,
        own_rows=own_rows,
        own_cross=own_cross,
        relay=relay,
        relay_back=relay_back,
        wrap_late=wrap_late,
        given=given,
        pass_on=pass_on_both,
        consume=consume,
        clear=clear,
    )
    count = chunks * PARTS

    def step(t, carry):
        for name in ORDER:
            q = t - LATER[name]

            @pl.when(jnp.logical_and(q >= 0, q < count))
            def _(name=name, q=q):
                actions[name](q // PARTS, lax.rem(q, PARTS))

        return carry

    lax.fori_loop(0, count + max(LATER.values()), step, 0)

    for flow in range(6):
        pltpu.make_async_remote_copy(
            src_ref=transit,
            dst_ref=transit,
            send_sem=s_sem.at[flow],
            recv_sem=r_transit.at[0, 0, 0],
            device_id=twin,
            device_id_type=MESH,
        ).wait_send()


def finish(half, scale, acc, r_hi, r_lo, l_hi, l_lo, out_ref, total, sem):
    every = tiles(acc.shape[1])
    early = early_tiles(acc.shape[1], half)
    copies = []

    def write(source, where):
        for b in range(5):
            start, stop = max(where.start, b * half), min(where.start + where.size, (b + 1) * half)
            if start < stop:
                target = out_ref.at[b, :, pl.ds(start - b * half, stop - start)]
                copies.append(pltpu.make_async_copy(source.at[:, pl.ds(start, stop - start)], target, sem.at[len(copies)]))
                copies[-1].start()

    for where in every:
        if where in early:
            write(acc, where)
    for where in every:
        if where not in early:
            total[:, where] = acc[:, where] + product(l_hi, l_lo, r_hi, r_lo, where) * scale
            write(total, where)
    for copy in copies:
        copy.wait()


def local(samples):
    count, width = samples.shape
    feats = lax.axis_size("feat")
    half, chunks = count // feats, width // LANES
    scale = float(1.0 / (width * feats) ** 0.5)
    block = (half, LANES)
    parts = pl.pallas_call(
        functools.partial(kernel, lax.axis_size("blk"), chunks, half, scale),
        out_shape=[
            pltpu.VMEM((count, 5 * half), jnp.float32),
            pltpu.VMEM((5 * half, 2 * LANES), jnp.bfloat16),
            pltpu.VMEM((5 * half, 2 * LANES), jnp.bfloat16),
            pltpu.VMEM((count, 2 * LANES), jnp.bfloat16),
            pltpu.VMEM((count, 2 * LANES), jnp.bfloat16),
        ],
        in_specs=[pl.BlockSpec(memory_space=pltpu.HBM)],
        out_specs=[pl.BlockSpec(memory_space=pltpu.VMEM)] * 5,
        scratch_shapes=[
            pltpu.VMEM((5, 2, chunks, *block), jnp.float32),
            pltpu.VMEM((2, chunks, *block), jnp.float32),
            pltpu.VMEM((2, chunks, *block), jnp.float32),
            pltpu.SemaphoreType.DMA((5, 2, chunks, PARTS)),
            pltpu.SemaphoreType.DMA((2, chunks, PARTS)),
            pltpu.SemaphoreType.DMA((2, chunks, PARTS)),
            pltpu.SemaphoreType.DMA((6,)),
            pltpu.SemaphoreType.REGULAR,
        ],
        compiler_params=pltpu.CompilerParams(collective_id=0, has_side_effects=True, vmem_limit_bytes=54 * 1024 * 1024),
        name="banded_gram",
    )(samples)
    return pl.pallas_call(
        functools.partial(finish, half, scale),
        out_shape=jax.ShapeDtypeStruct((5, count, half), jnp.float32),
        in_specs=[pl.BlockSpec(memory_space=pltpu.VMEM)] * 5,
        out_specs=pl.BlockSpec(memory_space=pltpu.HBM),
        scratch_shapes=[pltpu.VMEM((count, 5 * half), jnp.float32), pltpu.SemaphoreType.DMA((16,))],
        compiler_params=pltpu.CompilerParams(vmem_limit_bytes=16 * 1024 * 1024),
        name="finish",
    )(*parts)


def solution(mesh):
    in_specs = (P("blk", "feat"),)
    out_specs = P(None, "blk", "feat")
    return jax.shard_map(local, mesh=mesh, in_specs=in_specs, out_specs=out_specs, check_vma=False)
```
